32 devices in a mesh: groups: 2 (over y), prompt: 4 (over z), sample: 2 (over x), head: 2 (over core).
Axes of the slice: x: 2, y: 2, z: 4, core: 2. Of those that a mesh axis runs over, the one named last changes fastest.
Arguments:
- queries: bfloat16 [256, 16, 576], P(('groups', 'prompt', 'sample'), 'head'), parts along dimension 0, may hold values from -6 to 6
- prompt_cache: bfloat16 [16, 1024, 576], P(('groups', 'prompt'), 'sample'), parts along dimension 0, may hold values from -6 to 6
- suffix_cache: bfloat16 [256, 64, 576], P(('groups', 'prompt', 'sample')), parts along dimension 0, may hold values from -6 to 6
- suffix_len: int32 [256], P(('groups', 'prompt', 'sample')), parts along dimension 0, may hold values from 2 to 64, as said below
- sample_prompt: int32 [256], P('groups'), parts along dimension 0, may hold values from 0 to 7, as said below
- prompt_slot: int32 [16], P('groups'), parts along dimension 0, may hold values from 0 to 7, as said below
Outputs:
- attended: bfloat16 [256, 16, 512], P(('groups', 'prompt', 'sample'), 'head'), parts along dimension 0
The draws below stay inside these ranges and needn't reach their ends.
There are 2 independent parts, one for each index of `groups`. The reference program is written for one: setup_inputs(seed, part) draws one part's arguments, and reference() takes and returns one part's arrays. A program takes and returns all parts, laid end to end along the dimension named above; each array names one. Nothing has to cross between parts.
Inputs may be any that keep to these rules, and one draw needn't show every extreme that they name: `suffix_len`: the value 64 is reached. Every prompt is named by exactly 16 samples; in each aligned block of 16 samples, prompt_slot[sample_prompt] // 2 takes no value more than 4 times, and some value exactly 4 times. `prompt_slot`: a permutation.
All inputs are finite; a program needn't handle non-finite values.
Results may differ from the reference program's by a relative error of at most 0.013.
Values may be sent and summed in bfloat16 or wider, within the bound.
A program may use at most 64 MiB of HBM per device.

```python
import math
import jax
import jax.numpy as jnp
from jax import lax

H = 16
DL = 512
DR = 64
QKN = 128
SPP = 16
P_DEV = 2
PTOK = 1024
SUF = 64
PROMPTS = 8
S_DEV = 16
SAMPLES = 128


def base_field(key, shape):
    return jax.random.truncated_normal(key, -6.0, 6.0, shape, jnp.float32)


def keyed_field(key, salt, shape):
    field = base_field(jax.random.fold_in(key, salt), shape)
    return field.astype(jnp.bfloat16)


def draw_queries(key, part):
    field = base_field(jax.random.fold_in(key, 31), (SAMPLES, H, DL + DR))
    return field.astype(jnp.bfloat16)


def draw_prompt_cache(key, part):
    return keyed_field(key, 61, (PROMPTS, PTOK, DL + DR))


def draw_suffix_cache(key, part):
    return keyed_field(key, 71, (SAMPLES, SUF, DL + DR))


def draw_suffix_len(key, part):
    lengths = jax.random.randint(jax.random.fold_in(key, 51), (SAMPLES,), 2, SUF + 1)
    return lengths.at[0].set(SUF).astype(jnp.int32)


def routing_draw(key):
    owner_count = PROMPTS // P_DEV
    device_count = SAMPLES // S_DEV
    prompt_slot = jax.random.permutation(jax.random.fold_in(key, 41), PROMPTS)
    seats = jnp.repeat(jnp.arange(P_DEV, dtype=jnp.int32), SPP)
    owner_keys = jax.random.split(jax.random.fold_in(key, 42), owner_count)
    shuffled = jax.vmap(lambda single: jax.random.permutation(single, seats))(owner_keys)
    slots = (jnp.arange(owner_count, dtype=jnp.int32)[:, None] * P_DEV + shuffled).reshape(-1)
    dealt = slots.reshape(S_DEV, device_count).T
    device_order = jax.random.permutation(jax.random.fold_in(key, 44), device_count)
    per_device = dealt[jnp.argsort(device_order)]
    device_keys = jax.random.split(jax.random.fold_in(key, 43), device_count)
    orders = jax.vmap(lambda single: jax.random.permutation(single, S_DEV))(device_keys)
    per_device = jnp.take_along_axis(per_device, orders, axis=1)
    inverse = jnp.argsort(prompt_slot)
    sample_prompt = inverse[per_device.reshape(-1)]
    return (sample_prompt.astype(jnp.int32), prompt_slot.astype(jnp.int32))


def draw_sample_prompt(key, part):
    return routing_draw(key)[0]


def draw_prompt_slot(key, part):
    return routing_draw(key)[1]


def setup_inputs(seed: int = 0, part: int = 0) -> dict:
    seeds = jax.random.split(jax.random.key(seed), 7)
    own_keys = jax.random.split(jax.random.fold_in(seeds[6], part), 7)
    return {
        "queries": draw_queries(jax.random.fold_in(jax.random.fold_in(seeds[6], part), 71), part),
        "prompt_cache": draw_prompt_cache(jax.random.fold_in(jax.random.fold_in(seeds[6], part), 71), part),
        "suffix_cache": draw_suffix_cache(jax.random.fold_in(jax.random.fold_in(seeds[6], part), 71), part),
        "suffix_len": draw_suffix_len(jax.random.fold_in(jax.random.fold_in(seeds[6], part), 71), part),
        "sample_prompt": draw_sample_prompt(jax.random.fold_in(jax.random.fold_in(seeds[6], part), 71), part),
        "prompt_slot": draw_prompt_slot(jax.random.fold_in(jax.random.fold_in(seeds[6], part), 71), part),
    }


def reference(queries, prompt_cache, suffix_cache, suffix_len, sample_prompt, prompt_slot):
    scaling = 1.0 / math.sqrt(QKN + DR)
    members = jnp.argsort(sample_prompt, stable=True).astype(jnp.int32).reshape(PROMPTS, SPP)

    def per_prompt(prompt):
        chosen = members[prompt]
        asked = queries[chosen].astype(jnp.float32)
        shared = prompt_cache[prompt_slot[prompt]].astype(jnp.float32)
        recent = suffix_cache[chosen].astype(jnp.float32)
        lengths = suffix_len[chosen]
        shared_scores = jnp.einsum('shf,tf->sht', asked, shared) * scaling
        recent_scores = jnp.einsum('shf,stf->sht', asked, recent) * scaling
        allowed = jnp.arange(SUF, dtype=jnp.int32)[None, :] < lengths[:, None]
        recent_scores = jnp.where(allowed[:, None, :], recent_scores, -1e+30)
        row_max = jnp.maximum(lax.optimization_barrier(jnp.max(shared_scores, axis=-1)), lax.optimization_barrier(jnp.max(recent_scores, axis=-1)))
        shared_weights = jnp.exp(shared_scores - row_max[..., None])
        recent_weights = jnp.exp(recent_scores - row_max[..., None])
        row_sum = lax.optimization_barrier(jnp.sum(shared_weights, axis=-1)) + lax.optimization_barrier(jnp.sum(recent_weights, axis=-1))
        shared_rounded = lax.optimization_barrier(shared_weights.astype(jnp.bfloat16)).astype(jnp.float32)
        recent_rounded = lax.optimization_barrier(recent_weights.astype(jnp.bfloat16)).astype(jnp.float32)
        mixed = jnp.einsum('sht,td->shd', shared_rounded, shared[:, :DL])
        mixed = mixed + jnp.einsum('sht,std->shd', recent_rounded, recent[:, :, :DL])
        return (mixed / row_sum[..., None]).astype(jnp.bfloat16)
    results = lax.map(per_prompt, jnp.arange(PROMPTS, dtype=jnp.int32))
    output = jnp.zeros((SAMPLES, H, DL), jnp.bfloat16)
    return output.at[members.reshape(-1)].set(results.reshape(SAMPLES, H, DL))
```

```python
import functools
import math

import jax
import jax.numpy as jnp
from jax import lax
from jax.experimental import pallas as pl
from jax.experimental.pallas import tpu as pltpu
from jax.sharding import PartitionSpec as P

DL = 512
DR = 64
QKN = 128
LANES = 128
TILE_ROWS = 128
LOG2E = 1.4426950408889634
MESH = pl.DeviceIdType.MESH
F32 = jnp.float32
BF16 = jnp.bfloat16


def dot_t(a, b):
    return lax.dot_general(a, b, (((1,), (1,)), ((), ())), preferred_element_type=F32)


def dot(a, b):
    return lax.dot_general(a, b, (((1,), (0,)), ((), ())), preferred_element_type=F32)


def split3(x):
    hi = x.astype(BF16)
    left = x - hi.astype(F32)
    mid = left.astype(BF16)
    low = (left - mid.astype(F32)).astype(BF16)
    return hi, mid, low


def kernel(
    nz,
    nx,
    own_count,
    heads,
    sends,
    q_ref,
    kv_hbm,
    suf_hbm,
    len_ref,
    sp_ref,
    slot_ref,
    out_ref,
    packed,
    recv,
    ret,
    got,
    kbuf,
    sbuf,
    unpack,
    suf_out,
    result,
    local_sem,
    q_send,
    q_recv,
    r_send,
    r_recv,
):
    z = lax.axis_index("prompt")
    x = lax.axis_index("sample")
    prompts, tokens, features = kbuf.shape
    suffix = sbuf.shape[0] // own_count
    rows = sends * heads
    cols = own_count * heads
    packed_rows = nz * rows
    factor = LOG2E / math.sqrt(QKN + DR)
    pairs = [(dz, dx) for dz in range(nz) for dx in range(nx)]
    pairs.sort(key=lambda p: (min(p[0], nz - p[0]) + min(p[1], nx - p[1]), p))

    def ahead(dz, dx):
        return {"prompt": lax.rem(z + dz, nz), "sample": lax.rem(x + dx, nx)}

    def behind(dz, dx):
        return {"prompt": lax.rem(z + nz - dz, nz), "sample": lax.rem(x + nx - dx, nx)}

    barrier = pltpu.get_barrier_semaphore()
    for dz, dx in pairs[1:]:
        pl.semaphore_signal(barrier, inc=1, device_id=ahead(dz, dx), device_id_type=MESH)
    suf_copy = pltpu.make_async_copy(suf_hbm, sbuf, local_sem.at[0])
    suf_copy.start()
    kv_copy = pltpu.make_async_copy(kv_hbm, kbuf, local_sem.at[1])
    kv_copy.start()

    first = (z * nx + x) * own_count
    lane = lax.broadcasted_iota(jnp.int32, (own_count, cols), 1)
    row = lax.broadcasted_iota(jnp.int32, (own_count, cols), 0)
    owner_row = jnp.zeros((own_count, cols), jnp.int32)
    owner_lane = jnp.zeros((own_count, cols), jnp.int32)
    lane1 = lane[:1]
    local_lane = jnp.zeros((1, cols), jnp.int32)
    len_lane = jnp.zeros((1, cols), jnp.int32)
    lo_lane = jnp.zeros((1, cols), jnp.int32)
    sample_lane = jnp.zeros((own_count, cols), jnp.int32)
    for j in range(own_count):
        slot = slot_ref[sp_ref[first + j]]
        owner = lax.rem(lax.div(slot, prompts) - z + nz, nz)
        here = (lane >= j * heads) & (lane < (j + 1) * heads)
        owner_row = jnp.where(row == j, owner, owner_row)
        owner_lane = jnp.where(here, owner, owner_lane)
        sample_lane = jnp.where(here, j, sample_lane)
        local_lane = jnp.where(here[:1], lax.rem(slot, prompts), local_lane)
        len_lane = jnp.where(here[:1], len_ref[j], len_lane)
        lo_lane = jnp.where(here[:1], j * suffix, lo_lane)
    earlier = (owner_row == owner_lane) & (row < sample_lane)
    rank = jnp.sum(jnp.where(earlier, 1.0, 0.0), axis=0, keepdims=True).astype(jnp.int32)
    place = (owner_lane[:1] * sends + rank) * heads + (lane1 - sample_lane[:1] * heads)
    hot = lax.broadcasted_iota(jnp.int32, (packed_rows, cols), 0) == place

    def to_rows(values):
        return jnp.sum(jnp.where(hot, values.astype(F32), 0.0), axis=1, keepdims=True)

    hot_f = jnp.where(hot, 1.0, 0.0)
    mine = dot(hot_f.astype(BF16), q_ref[...]).astype(BF16)
    tail = jnp.broadcast_to(to_rows(local_lane), (packed_rows, LANES)).astype(BF16)
    packed[:, :features] = mine
    packed[:, features:] = tail[:, : packed.shape[1] - features]
    recv[:rows] = packed[:rows]

    pl.semaphore_wait(barrier, nz * nx - 1)
    q_copies = []
    for k, (dz, dx) in enumerate(pairs):
        if k == 0:
            q_copies.append(None)
            continue
        copy = pltpu.make_async_remote_copy(
            src_ref=packed.at[pl.ds(dz * rows, rows)],
            dst_ref=recv.at[pl.ds(k * rows, rows)],
            send_sem=q_send.at[k],
            recv_sem=q_recv.at[k],
            device_id=ahead(dz, dx),
            device_id_type=MESH,
        )
        copy.start()
        q_copies.append(copy)

    unpack[...] = hot_f.T.astype(BF16)
    lo = to_rows(lo_lane).astype(jnp.int32)
    hi = to_rows(lo_lane + len_lane).astype(jnp.int32)
    suf_copy.wait()
    scores = dot_t(packed[:, :features], sbuf[...]) * factor
    key = lax.broadcasted_iota(jnp.int32, scores.shape, 1)
    scores = jnp.where((key >= lo) & (key < hi), scores, -1e30)
    suf_max = jnp.max(scores, axis=1, keepdims=True)
    weights = jnp.exp2(scores - suf_max)
    suf_sum = jnp.sum(weights, axis=1, keepdims=True)
    suf_out[...] = dot(weights.astype(BF16), sbuf[:, :DL])

    kv_copy.wait()
    step = max(1, TILE_ROWS // rows)
    r_copies = [None] * len(pairs)
    for begin in range(0, len(pairs), step):
        end = min(begin + step, len(pairs))
        for k in range(begin, end):
            if k:
                q_copies[k].wait_recv()
        span = pl.ds(begin * rows, (end - begin) * rows)
        asked = recv[span, :features]
        local = recv[span, features : features + 1].astype(F32)
        scores = dot_t(asked, kbuf[0])
        for p in range(1, prompts):
            scores = jnp.where(local == float(p), dot_t(asked, kbuf[p]), scores)
        scores = scores * factor
        row_max = jnp.max(scores, axis=1, keepdims=True)
        weights = jnp.exp2(scores - row_max)
        row_sum = jnp.sum(weights, axis=1, keepdims=True)
        total = None
        for p in range(prompts):
            part = jnp.where(local == float(p), weights, 0.0).astype(BF16)
            part = dot(part, kbuf[p, :, :DL])
            total = part if total is None else total + part
        lse = row_max + jnp.log(row_sum) * LOG2E
        ret[span, :DL] = (total / row_sum).astype(BF16)
        place_of = lax.broadcasted_iota(jnp.int32, ((end - begin) * rows, LANES), 1)
        top, mid, low = split3(lse)
        tail = jnp.where(place_of == 0, top.astype(F32), jnp.where(place_of == 1, mid.astype(F32), low.astype(F32)))
        ret[span, DL:] = tail.astype(BF16)
        for k in range(begin, end):
            dz, dx = pairs[k]
            if k == 0:
                got[:rows] = ret[:rows]
                continue
            copy = pltpu.make_async_remote_copy(
                src_ref=ret.at[pl.ds(k * rows, rows)],
                dst_ref=got.at[pl.ds(k * rows, rows)],
                send_sem=r_send.at[k],
                recv_sem=r_recv.at[k],
                device_id=behind(dz, dx),
                device_id_type=MESH,
            )
            copy.start()
            r_copies[k] = copy

    for k in range(1, len(pairs)):
        r_copies[k].wait_recv()
    for dz in range(nz):
        span = pl.ds(dz * rows, rows)
        at = slice(dz * rows, (dz + 1) * rows)
        parts = []
        top = suf_max[at]
        for k, pair in enumerate(pairs):
            if pair[0] == dz:
                tail = got[pl.ds(k * rows, rows), DL:].astype(F32)
                lse = tail[:, 0:1] + tail[:, 1:2] + tail[:, 2:3]
                parts.append((k, lse))
                top = jnp.maximum(top, lse)
        share = jnp.exp2(suf_max[at] - top)
        total = share * suf_sum[at]
        numerator = share * suf_out[span, :]
        for k, lse in parts:
            share = jnp.exp2(lse - top)
            total = total + share
            numerator = numerator + share * got[pl.ds(k * rows, rows), :DL].astype(F32)
        result[span, :] = (numerator / total).astype(BF16)
    out_ref[...] = dot(unpack[...], result[...]).astype(BF16)
    for k in range(1, len(pairs)):
        q_copies[k].wait_send()
        r_copies[k].wait_send()


def body(nz, nx, queries, prompt_cache, suffix_cache, suffix_len, sample_prompt, prompt_slot):
    own_count, heads, features = queries.shape
    prompts, tokens, _ = prompt_cache.shape
    suffix = suffix_cache.shape[1]
    sends = max(1, own_count // nz)
    devices = nz * nx
    cols = own_count * heads
    packed_rows = nz * sends * heads
    all_rows = devices * sends * heads
    wide = pl.cdiv(features + 1, LANES) * LANES
    vmem = pl.BlockSpec(memory_space=pltpu.VMEM)
    smem = pl.BlockSpec(memory_space=pltpu.SMEM)
    hbm = pl.BlockSpec(memory_space=pl.ANY)
    out = pl.pallas_call(
        functools.partial(kernel, nz, nx, own_count, heads, sends),
        out_shape=jax.ShapeDtypeStruct((cols, DL), BF16),
        in_specs=[vmem, hbm, hbm, smem, smem, smem],
        out_specs=vmem,
        scratch_shapes=[
            pltpu.VMEM((packed_rows, wide), BF16),
            pltpu.VMEM((all_rows, wide), BF16),
            pltpu.VMEM((all_rows, DL + LANES), BF16),
            pltpu.VMEM((all_rows, DL + LANES), BF16),
            pltpu.VMEM((prompts, tokens, features), BF16),
            pltpu.VMEM((own_count * suffix, features), BF16),
            pltpu.VMEM((cols, packed_rows), BF16),
            pltpu.VMEM((packed_rows, DL), F32),
            pltpu.VMEM((packed_rows, DL), BF16),
            pltpu.SemaphoreType.DMA((2,)),
            pltpu.SemaphoreType.DMA((devices,)),
            pltpu.SemaphoreType.DMA((devices,)),
            pltpu.SemaphoreType.DMA((devices,)),
            pltpu.SemaphoreType.DMA((devices,)),
        ],
        compiler_params=pltpu.CompilerParams(collective_id=0, has_side_effects=True),
        name="latent_decode",
    )(
        queries.reshape(cols, features),
        prompt_cache,
        suffix_cache.reshape(own_count * suffix, features),
        suffix_len,
        sample_prompt,
        prompt_slot,
    )
    return out.reshape(own_count, heads, DL)


def solution(mesh):
    return jax.shard_map(
        functools.partial(body, mesh.shape["prompt"], mesh.shape["sample"]),
        mesh=mesh,
        in_specs=(
            P(("groups", "prompt", "sample"), "head", None),
            P(("groups", "prompt"), "sample", None),
            P(("groups", "prompt", "sample"), None, None),
            P(("groups", "prompt", "sample")),
            P("groups"),
            P("groups"),
        ),
        out_specs=P(("groups", "prompt", "sample"), "head", None),
        check_vma=False,
    )
```

```python
import functools
import math

import jax
import jax.numpy as jnp
from jax import lax
from jax.experimental import pallas as pl
from jax.experimental.pallas import tpu as pltpu
from jax.sharding import PartitionSpec as P

DL = 512
DR = 64
QKN = 128
LANES = 128
TILE_ROWS = 128
LOG2E = 1.4426950408889634
MESH = pl.DeviceIdType.MESH
F32 = jnp.float32
BF16 = jnp.bfloat16


def dot_t(a, b):
    return lax.dot_general(a, b, (((1,), (1,)), ((), ())), preferred_element_type=F32)


def dot(a, b):
    return lax.dot_general(a, b, (((1,), (0,)), ((), ())), preferred_element_type=F32)


def split3(x):
    hi = x.astype(BF16)
    left = x - hi.astype(F32)
    mid = left.astype(BF16)
    low = (left - mid.astype(F32)).astype(BF16)
    return hi, mid, low


def kernel(
    nz,
    nx,
    own_count,
    heads,
    sends,
    q_ref,
    kv_hbm,
    suf_hbm,
    len_ref,
    sp_ref,
    slot_ref,
    out_ref,
    packed,
    recv,
    ret,
    got,
    kbuf,
    sbuf,
    unpack,
    suf_out,
    result,
    local_sem,
    q_send,
    q_recv,
    r_send,
    r_recv,
):
    z = lax.axis_index("prompt")
    x = lax.axis_index("sample")
    prompts, features, tokens = kbuf.shape
    suffix = sbuf.shape[0] // own_count
    rows = sends * heads
    cols = own_count * heads
    packed_rows = nz * rows
    factor = LOG2E / math.sqrt(QKN + DR)
    pairs = [(dz, dx) for dz in range(nz) for dx in range(nx)]
    pairs.sort(key=lambda p: (-min(p[0], nz - p[0]) - min(p[1], nx - p[1]), p))

    def ahead(dz, dx):
        return {"prompt": lax.rem(z + dz, nz), "sample": lax.rem(x + dx, nx)}

    def behind(dz, dx):
        return {"prompt": lax.rem(z + nz - dz, nz), "sample": lax.rem(x + nx - dx, nx)}

    barrier = pltpu.get_barrier_semaphore()
    for dz, dx in pairs[:-1]:
        pl.semaphore_signal(barrier, inc=1, device_id=ahead(dz, dx), device_id_type=MESH)
    suf_copy = pltpu.make_async_copy(suf_hbm, sbuf, local_sem.at[0])
    suf_copy.start()
    kv_copy = pltpu.make_async_copy(kv_hbm, kbuf, local_sem.at[1])
    kv_copy.start()

    first = (z * nx + x) * own_count
    lane = lax.broadcasted_iota(jnp.int32, (own_count, cols), 1)
    row = lax.broadcasted_iota(jnp.int32, (own_count, cols), 0)
    owner_row = jnp.zeros((own_count, cols), jnp.int32)
    owner_lane = jnp.zeros((own_count, cols), jnp.int32)
    lane1 = lane[:1]
    local_lane = jnp.zeros((1, cols), jnp.int32)
    len_lane = jnp.zeros((1, cols), jnp.int32)
    lo_lane = jnp.zeros((1, cols), jnp.int32)
    sample_lane = jnp.zeros((own_count, cols), jnp.int32)
    for j in range(own_count):
        slot = slot_ref[sp_ref[first + j]]
        owner = lax.rem(lax.div(slot, prompts) - z + nz, nz)
        here = (lane >= j * heads) & (lane < (j + 1) * heads)
        owner_row = jnp.where(row == j, owner, owner_row)
        owner_lane = jnp.where(here, owner, owner_lane)
        sample_lane = jnp.where(here, j, sample_lane)
        local_lane = jnp.where(here[:1], lax.rem(slot, prompts), local_lane)
        len_lane = jnp.where(here[:1], len_ref[j], len_lane)
        lo_lane = jnp.where(here[:1], j * suffix, lo_lane)
    earlier = (owner_row == owner_lane) & (row < sample_lane)
    rank = jnp.sum(jnp.where(earlier, 1.0, 0.0), axis=0, keepdims=True).astype(jnp.int32)
    place = (owner_lane[:1] * sends + rank) * heads + (lane1 - sample_lane[:1] * heads)
    hot = lax.broadcasted_iota(jnp.int32, (packed_rows, cols), 0) == place

    def to_rows(values):
        return jnp.sum(jnp.where(hot, values.astype(F32), 0.0), axis=1, keepdims=True)

    hot_f = jnp.where(hot, 1.0, 0.0)
    mine = dot(hot_f.astype(BF16), q_ref[...]).astype(BF16)
    tail = jnp.broadcast_to(to_rows(local_lane), (packed_rows, LANES)).astype(BF16)
    packed[:, :features] = mine
    packed[:, features:] = tail[:, : packed.shape[1] - features]
    recv[pl.ds((len(pairs) - 1) * rows, rows)] = packed[:rows]

    pl.semaphore_wait(barrier, nz * nx - 1)
    q_copies = []
    for k, (dz, dx) in enumerate(pairs):
        if k == len(pairs) - 1:
            q_copies.append(None)
            continue
        copy = pltpu.make_async_remote_copy(
            src_ref=packed.at[pl.ds(dz * rows, rows)],
            dst_ref=recv.at[pl.ds(k * rows, rows)],
            send_sem=q_send.at[k],
            recv_sem=q_recv.at[k],
            device_id=ahead(dz, dx),
            device_id_type=MESH,
        )
        copy.start()
        q_copies.append(copy)

    unpack[...] = hot_f.T.astype(BF16)
    lo = to_rows(lo_lane).astype(jnp.int32)
    hi = to_rows(lo_lane + len_lane).astype(jnp.int32)
    suf_copy.wait()
    scores = dot_t(packed[:, :features], sbuf[...]) * factor
    key = lax.broadcasted_iota(jnp.int32, scores.shape, 1)
    scores = jnp.where((key >= lo) & (key < hi), scores, -1e30)
    suf_max = jnp.max(scores, axis=1, keepdims=True)
    weights = jnp.exp2(scores - suf_max)
    suf_sum = jnp.sum(weights, axis=1, keepdims=True)
    suf_out[...] = dot(weights.astype(BF16), sbuf[:, :DL])

    kv_copy.wait()
    step = max(1, TILE_ROWS // rows)
    r_copies = [None] * len(pairs)
    for begin in range(0, len(pairs), step):
        end = min(begin + step, len(pairs))
        for k in range(begin, end):
            if k < len(pairs) - 1:
                q_copies[k].wait_recv()
        span = pl.ds(begin * rows, (end - begin) * rows)
        asked = recv[span, :features]
        local = recv[span, features : features + 1].astype(F32)
        scores = dot(asked, kbuf[0])
        for p in range(1, prompts):
            scores = jnp.where(local == float(p), dot(asked, kbuf[p]), scores)
        scores = scores * factor
        row_max = jnp.max(scores, axis=1, keepdims=True)
        weights = jnp.exp2(scores - row_max)
        row_sum = jnp.sum(weights, axis=1, keepdims=True)
        total = None
        for p in range(prompts):
            part = jnp.where(local == float(p), weights, 0.0).astype(BF16)
            part = dot_t(part, kbuf[p, :DL, :])
            total = part if total is None else total + part
        lse = row_max + jnp.log(row_sum) * LOG2E
        ret[span, :DL] = (total / row_sum).astype(BF16)
        place_of = lax.broadcasted_iota(jnp.int32, ((end - begin) * rows, LANES), 1)
        top, mid, low = split3(lse)
        tail = jnp.where(place_of == 0, top.astype(F32), jnp.where(place_of == 1, mid.astype(F32), low.astype(F32)))
        ret[span, DL:] = tail.astype(BF16)
        for k in range(begin, end):
            dz, dx = pairs[k]
            if k == len(pairs) - 1:
                got[pl.ds(k * rows, rows)] = ret[pl.ds(k * rows, rows)]
                continue
            copy = pltpu.make_async_remote_copy(
                src_ref=ret.at[pl.ds(k * rows, rows)],
                dst_ref=got.at[pl.ds(k * rows, rows)],
                send_sem=r_send.at[k],
                recv_sem=r_recv.at[k],
                device_id=behind(dz, dx),
                device_id_type=MESH,
            )
            copy.start()
            r_copies[k] = copy

    for k in range(len(pairs) - 1):
        r_copies[k].wait_recv()
    for dz in range(nz):
        span = pl.ds(dz * rows, rows)
        at = slice(dz * rows, (dz + 1) * rows)
        parts = []
        top = suf_max[at]
        for k, pair in enumerate(pairs):
            if pair[0] == dz:
                tail = got[pl.ds(k * rows, rows), DL:].astype(F32)
                lse = tail[:, 0:1] + tail[:, 1:2] + tail[:, 2:3]
                parts.append((k, lse))
                top = jnp.maximum(top, lse)
        share = jnp.exp2(suf_max[at] - top)
        total = share * suf_sum[at]
        numerator = share * suf_out[span, :]
        for k, lse in parts:
            share = jnp.exp2(lse - top)
            total = total + share
            numerator = numerator + share * got[pl.ds(k * rows, rows), :DL].astype(F32)
        result[span, :] = (numerator / total).astype(BF16)
    out_ref[...] = dot(unpack[...], result[...]).astype(BF16)
    for k in range(len(pairs) - 1):
        q_copies[k].wait_send()
        r_copies[k].wait_send()


def body(nz, nx, queries, prompt_cache, suffix_cache, suffix_len, sample_prompt, prompt_slot):
    own_count, heads, features = queries.shape
    prompts, tokens, _ = prompt_cache.shape
    suffix = suffix_cache.shape[1]
    sends = max(1, own_count // nz)
    devices = nz * nx
    cols = own_count * heads
    packed_rows = nz * sends * heads
    all_rows = devices * sends * heads
    wide = pl.cdiv(features + 1, LANES) * LANES
    vmem = pl.BlockSpec(memory_space=pltpu.VMEM)
    smem = pl.BlockSpec(memory_space=pltpu.SMEM)
    hbm = pl.BlockSpec(memory_space=pl.ANY)
    out = pl.pallas_call(
        functools.partial(kernel, nz, nx, own_count, heads, sends),
        out_shape=jax.ShapeDtypeStruct((cols, DL), BF16),
        in_specs=[vmem, hbm, hbm, smem, smem, smem],
        out_specs=vmem,
        scratch_shapes=[
            pltpu.VMEM((packed_rows, wide), BF16),
            pltpu.VMEM((all_rows, wide), BF16),
            pltpu.VMEM((all_rows, DL + LANES), BF16),
            pltpu.VMEM((all_rows, DL + LANES), BF16),
            pltpu.VMEM((prompts, features, tokens), BF16),
            pltpu.VMEM((own_count * suffix, features), BF16),
            pltpu.VMEM((cols, packed_rows), BF16),
            pltpu.VMEM((packed_rows, DL), F32),
            pltpu.VMEM((packed_rows, DL), BF16),
            pltpu.SemaphoreType.DMA((2,)),
            pltpu.SemaphoreType.DMA((devices,)),
            pltpu.SemaphoreType.DMA((devices,)),
            pltpu.SemaphoreType.DMA((devices,)),
            pltpu.SemaphoreType.DMA((devices,)),
        ],
        compiler_params=pltpu.CompilerParams(collective_id=0, has_side_effects=True),
        name="latent_decode",
    )(
        queries.reshape(cols, features),
        jnp.swapaxes(prompt_cache, 1, 2),
        suffix_cache.reshape(own_count * suffix, features),
        suffix_len,
        sample_prompt,
        prompt_slot,
    )
    return out.reshape(own_count, heads, DL)


def solution(mesh):
    return jax.shard_map(
        functools.partial(body, mesh.shape["prompt"], mesh.shape["sample"]),
        mesh=mesh,
        in_specs=(
            P(("groups", "prompt", "sample"), "head", None),
            P(("groups", "prompt"), "sample", None),
            P(("groups", "prompt", "sample"), None, None),
            P(("groups", "prompt", "sample")),
            P("groups"),
            P("groups"),
        ),
        out_specs=P(("groups", "prompt", "sample"), "head", None),
        check_vma=False,
    )
```

```python
import functools
import math

import jax
import jax.numpy as jnp
from jax import lax
from jax.experimental import pallas as pl
from jax.experimental.pallas import tpu as pltpu
from jax.sharding import PartitionSpec as P

DL = 512
DR = 64
QKN = 128
LANES = 128
TILE_ROWS = 128
LOG2E = 1.4426950408889634
MESH = pl.DeviceIdType.MESH
F32 = jnp.float32
BF16 = jnp.bfloat16


def dot_t(a, b):
    return lax.dot_general(a, b, (((1,), (1,)), ((), ())), preferred_element_type=F32)


def dot(a, b):
    return lax.dot_general(a, b, (((1,), (0,)), ((), ())), preferred_element_type=F32)


def split3(x):
    hi = x.astype(BF16)
    left = x - hi.astype(F32)
    mid = left.astype(BF16)
    low = (left - mid.astype(F32)).astype(BF16)
    return hi, mid, low


def kernel(
    nz,
    nx,
    own_count,
    heads,
    sends,
    q_hbm,
    kv_hbm,
    suf_hbm,
    len_hbm,
    sp_hbm,
    slot_hbm,
    out_ref,
    packed,
    recv,
    ret,
    got,
    len_ref,
    sp_ref,
    slot_ref,
    q_ref,
    kbuf,
    sbuf,
    unpack,
    suf_out,
    result,
    local_sem,
    q_send,
    q_recv,
    r_send,
    r_recv,
):
    z = lax.axis_index("prompt")
    x = lax.axis_index("sample")
    prompts, features, tokens = kbuf.shape
    suffix = sbuf.shape[0] // own_count
    rows = sends * heads
    cols = own_count * heads
    packed_rows = nz * rows
    factor = LOG2E / math.sqrt(QKN + DR)
    pairs = [(dz, dx) for dz in range(nz) for dx in range(nx)]
    pairs.sort(key=lambda p: (-min(p[0], nz - p[0]) - min(p[1], nx - p[1]), p))

    def ahead(dz, dx):
        return {"prompt": lax.rem(z + dz, nz), "sample": lax.rem(x + dx, nx)}

    def behind(dz, dx):
        return {"prompt": lax.rem(z + nz - dz, nz), "sample": lax.rem(x + nx - dx, nx)}

    barrier = pltpu.get_barrier_semaphore()
    for dz, dx in pairs[:-1]:
        pl.semaphore_signal(barrier, inc=1, device_id=ahead(dz, dx), device_id_type=MESH)
    tables = [
        pltpu.make_async_copy(source, target, local_sem.at[3 + i])
        for i, (source, target) in enumerate(((slot_hbm, slot_ref), (sp_hbm, sp_ref), (len_hbm, len_ref)))
    ]
    for table in tables:
        table.start()
    q_load = pltpu.make_async_copy(q_hbm, q_ref, local_sem.at[2])
    q_load.start()
    suf_copy = pltpu.make_async_copy(suf_hbm, sbuf, local_sem.at[0])
    suf_copy.start()
    kv_copy = pltpu.make_async_copy(kv_hbm, kbuf, local_sem.at[1])
    kv_copy.start()

    for table in tables:
        table.wait()
    first = (z * nx + x) * own_count
    lane = lax.broadcasted_iota(jnp.int32, (own_count, cols), 1)
    row = lax.broadcasted_iota(jnp.int32, (own_count, cols), 0)
    owner_row = jnp.zeros((own_count, cols), jnp.int32)
    owner_lane = jnp.zeros((own_count, cols), jnp.int32)
    lane1 = lane[:1]
    local_lane = jnp.zeros((1, cols), jnp.int32)
    len_lane = jnp.zeros((1, cols), jnp.int32)
    lo_lane = jnp.zeros((1, cols), jnp.int32)
    sample_lane = jnp.zeros((own_count, cols), jnp.int32)
    for j in range(own_count):
        slot = slot_ref[sp_ref[first + j]]
        owner = lax.rem(lax.div(slot, prompts) - z + nz, nz)
        here = (lane >= j * heads) & (lane < (j + 1) * heads)
        owner_row = jnp.where(row == j, owner, owner_row)
        owner_lane = jnp.where(here, owner, owner_lane)
        sample_lane = jnp.where(here, j, sample_lane)
        local_lane = jnp.where(here[:1], lax.rem(slot, prompts), local_lane)
        len_lane = jnp.where(here[:1], len_ref[j], len_lane)
        lo_lane = jnp.where(here[:1], j * suffix, lo_lane)
    earlier = (owner_row == owner_lane) & (row < sample_lane)
    rank = jnp.sum(jnp.where(earlier, 1.0, 0.0), axis=0, keepdims=True).astype(jnp.int32)
    place = (owner_lane[:1] * sends + rank) * heads + (lane1 - sample_lane[:1] * heads)
    hot = lax.broadcasted_iota(jnp.int32, (packed_rows, cols), 0) == place

    def to_rows(values):
        return jnp.sum(jnp.where(hot, values.astype(F32), 0.0), axis=1, keepdims=True)

    hot_f = jnp.where(hot, 1.0, 0.0)
    q_load.wait()
    mine = dot(hot_f.astype(BF16), q_ref[...]).astype(BF16)
    tail = jnp.broadcast_to(to_rows(local_lane), (packed_rows, LANES)).astype(BF16)
    packed[:, :features] = mine
    packed[:, features:] = tail[:, : packed.shape[1] - features]
    recv[pl.ds((len(pairs) - 1) * rows, rows)] = packed[:rows]

    pl.semaphore_wait(barrier, nz * nx - 1)
    q_copies = []
    for k, (dz, dx) in enumerate(pairs):
        if k == len(pairs) - 1:
            q_copies.append(None)
            continue
        copy = pltpu.make_async_remote_copy(
            src_ref=packed.at[pl.ds(dz * rows, rows)],
            dst_ref=recv.at[pl.ds(k * rows, rows)],
            send_sem=q_send.at[k],
            recv_sem=q_recv.at[k],
            device_id=ahead(dz, dx),
            device_id_type=MESH,
        )
        copy.start()
        q_copies.append(copy)

    unpack[...] = hot_f.T.astype(BF16)
    lo = to_rows(lo_lane).astype(jnp.int32)
    hi = to_rows(lo_lane + len_lane).astype(jnp.int32)
    suf_copy.wait()
    scores = dot_t(packed[:, :features], sbuf[...]) * factor
    key = lax.broadcasted_iota(jnp.int32, scores.shape, 1)
    scores = jnp.where((key >= lo) & (key < hi), scores, -1e30)
    suf_max = jnp.max(scores, axis=1, keepdims=True)
    weights = jnp.exp2(scores - suf_max)
    suf_sum = jnp.sum(weights, axis=1, keepdims=True)
    suf_out[...] = dot(weights.astype(BF16), sbuf[:, :DL])

    kv_copy.wait()
    step = max(1, TILE_ROWS // rows)
    r_copies = [None] * len(pairs)
    for begin in range(0, len(pairs), step):
        end = min(begin + step, len(pairs))
        for k in range(begin, end):
            if k < len(pairs) - 1:
                q_copies[k].wait_recv()
        span = pl.ds(begin * rows, (end - begin) * rows)
        asked = recv[span, :features]
        local = recv[span, features : features + 1].astype(F32)
        scores = dot(asked, kbuf[0])
        for p in range(1, prompts):
            scores = jnp.where(local == float(p), dot(asked, kbuf[p]), scores)
        scores = scores * factor
        row_max = jnp.max(scores, axis=1, keepdims=True)
        weights = jnp.exp2(scores - row_max)
        row_sum = jnp.sum(weights, axis=1, keepdims=True)
        total = None
        for p in range(prompts):
            part = jnp.where(local == float(p), weights, 0.0).astype(BF16)
            part = dot_t(part, kbuf[p, :DL, :])
            total = part if total is None else total + part
        lse = row_max + jnp.log(row_sum) * LOG2E
        ret[span, :DL] = (total / row_sum).astype(BF16)
        place_of = lax.broadcasted_iota(jnp.int32, ((end - begin) * rows, LANES), 1)
        top, mid, low = split3(lse)
        tail = jnp.where(place_of == 0, top.astype(F32), jnp.where(place_of == 1, mid.astype(F32), low.astype(F32)))
        ret[span, DL:] = tail.astype(BF16)
        for k in range(begin, end):
            dz, dx = pairs[k]
            if k == len(pairs) - 1:
                got[pl.ds(k * rows, rows)] = ret[pl.ds(k * rows, rows)]
                continue
            copy = pltpu.make_async_remote_copy(
                src_ref=ret.at[pl.ds(k * rows, rows)],
                dst_ref=got.at[pl.ds(k * rows, rows)],
                send_sem=r_send.at[k],
                recv_sem=r_recv.at[k],
                device_id=behind(dz, dx),
                device_id_type=MESH,
            )
            copy.start()
            r_copies[k] = copy

    for k in range(len(pairs) - 1):
        r_copies[k].wait_recv()
    for dz in range(nz):
        span = pl.ds(dz * rows, rows)
        at = slice(dz * rows, (dz + 1) * rows)
        parts = []
        top = suf_max[at]
        for k, pair in enumerate(pairs):
            if pair[0] == dz:
                tail = got[pl.ds(k * rows, rows), DL:].astype(F32)
                lse = tail[:, 0:1] + tail[:, 1:2] + tail[:, 2:3]
                parts.append((k, lse))
                top = jnp.maximum(top, lse)
        share = jnp.exp2(suf_max[at] - top)
        total = share * suf_sum[at]
        numerator = share * suf_out[span, :]
        for k, lse in parts:
            share = jnp.exp2(lse - top)
            total = total + share
            numerator = numerator + share * got[pl.ds(k * rows, rows), :DL].astype(F32)
        result[span, :] = (numerator / total).astype(BF16)
    out_ref[...] = dot(unpack[...], result[...]).astype(BF16)
    for k in range(len(pairs) - 1):
        q_copies[k].wait_send()
        r_copies[k].wait_send()


def body(nz, nx, queries, prompt_cache, suffix_cache, suffix_len, sample_prompt, prompt_slot):
    own_count, heads, features = queries.shape
    prompts, tokens, _ = prompt_cache.shape
    suffix = suffix_cache.shape[1]
    sends = max(1, own_count // nz)
    devices = nz * nx
    cols = own_count * heads
    packed_rows = nz * sends * heads
    all_rows = devices * sends * heads
    wide = pl.cdiv(features + 1, LANES) * LANES
    vmem = pl.BlockSpec(memory_space=pltpu.VMEM)
    hbm = pl.BlockSpec(memory_space=pl.ANY)
    out = pl.pallas_call(
        functools.partial(kernel, nz, nx, own_count, heads, sends),
        out_shape=pltpu.VMEM((cols, DL), BF16),
        in_specs=[hbm] * 6,
        out_specs=vmem,
        scratch_shapes=[
            pltpu.VMEM((packed_rows, wide), BF16),
            pltpu.VMEM((all_rows, wide), BF16),
            pltpu.VMEM((all_rows, DL + LANES), BF16),
            pltpu.VMEM((all_rows, DL + LANES), BF16),
            pltpu.SMEM(suffix_len.shape, jnp.int32),
            pltpu.SMEM(sample_prompt.shape, jnp.int32),
            pltpu.SMEM(prompt_slot.shape, jnp.int32),
            pltpu.VMEM((cols, features), BF16),
            pltpu.VMEM((prompts, features, tokens), BF16),
            pltpu.VMEM((own_count * suffix, features), BF16),
            pltpu.VMEM((cols, packed_rows), BF16),
            pltpu.VMEM((packed_rows, DL), F32),
            pltpu.VMEM((packed_rows, DL), BF16),
            pltpu.SemaphoreType.DMA((6,)),
            pltpu.SemaphoreType.DMA((devices,)),
            pltpu.SemaphoreType.DMA((devices,)),
            pltpu.SemaphoreType.DMA((devices,)),
            pltpu.SemaphoreType.DMA((devices,)),
        ],
        compiler_params=pltpu.CompilerParams(collective_id=0, has_side_effects=True),
        name="latent_decode",
    )(
        queries.reshape(cols, features),
        jnp.swapaxes(prompt_cache, 1, 2),
        suffix_cache.reshape(own_count * suffix, features),
        suffix_len,
        sample_prompt,
        prompt_slot,
    )
    return out.reshape(own_count, heads, DL)


def solution(mesh):
    return jax.shard_map(
        functools.partial(body, mesh.shape["prompt"], mesh.shape["sample"]),
        mesh=mesh,
        in_specs=(
            P(("groups", "prompt", "sample"), "head", None),
            P(("groups", "prompt"), "sample", None),
            P(("groups", "prompt", "sample"), None, None),
            P(("groups", "prompt", "sample")),
            P("groups"),
            P("groups"),
        ),
        out_specs=P(("groups", "prompt", "sample"), "head", None),
        check_vma=False,
    )
```

```python
import functools
import math

import jax
import jax.numpy as jnp
from jax import lax
from jax.experimental import pallas as pl
from jax.experimental.pallas import tpu as pltpu
from jax.sharding import PartitionSpec as P

DL = 512
DR = 64
QKN = 128
LANES = 128
TILE_ROWS = 128
LOG2E = 1.4426950408889634
MESH = pl.DeviceIdType.MESH
F32 = jnp.float32
BF16 = jnp.bfloat16


def dot_t(a, b):
    return lax.dot_general(a, b, (((1,), (1,)), ((), ())), preferred_element_type=F32)


def dot(a, b):
    return lax.dot_general(a, b, (((1,), (0,)), ((), ())), preferred_element_type=F32)


def split3(x):
    hi = x.astype(BF16)
    left = x - hi.astype(F32)
    mid = left.astype(BF16)
    low = (left - mid.astype(F32)).astype(BF16)
    return hi, mid, low


def kernel(
    nz,
    nx,
    own_count,
    heads,
    sends,
    q_hbm,
    kv_hbm,
    suf_hbm,
    len_hbm,
    sp_hbm,
    slot_hbm,
    out_ref,
    packed,
    recv,
    ret,
    got,
    len_ref,
    sp_ref,
    slot_ref,
    q_ref,
    kbuf,
    sbuf,
    unpack,
    suf_out,
    result,
    local_sem,
    q_send,
    q_recv,
    r_send,
    r_recv,
):
    z = lax.axis_index("prompt")
    x = lax.axis_index("sample")
    prompts, features, tokens = kbuf.shape
    suffix = sbuf.shape[0] // own_count
    rows = sends * heads
    cols = own_count * heads
    packed_rows = nz * rows
    factor = LOG2E / math.sqrt(QKN + DR)
    pairs = [(dz, dx) for dz in range(nz) for dx in range(nx)]
    pairs.sort(key=lambda p: (-min(p[0], nz - p[0]), -min(p[1], nx - p[1]), p))

    def ahead(dz, dx):
        return {"prompt": lax.rem(z + dz, nz), "sample": lax.rem(x + dx, nx)}

    def behind(dz, dx):
        return {"prompt": lax.rem(z + nz - dz, nz), "sample": lax.rem(x + nx - dx, nx)}

    barrier = pltpu.get_barrier_semaphore()
    for dz, dx in pairs[:-1]:
        pl.semaphore_signal(barrier, inc=1, device_id=ahead(dz, dx), device_id_type=MESH)
    tables = [
        pltpu.make_async_copy(source, target, local_sem.at[3 + i])
        for i, (source, target) in enumerate(((slot_hbm, slot_ref), (sp_hbm, sp_ref), (len_hbm, len_ref)))
    ]
    for table in tables:
        table.start()
    q_load = pltpu.make_async_copy(q_hbm, q_ref, local_sem.at[2])
    q_load.start()
    suf_copy = pltpu.make_async_copy(suf_hbm, sbuf, local_sem.at[0])
    suf_copy.start()
    kv_copy = pltpu.make_async_copy(kv_hbm, kbuf, local_sem.at[1])
    kv_copy.start()

    for table in tables:
        table.wait()
    first = (z * nx + x) * own_count
    lane = lax.broadcasted_iota(jnp.int32, (own_count, cols), 1)
    row = lax.broadcasted_iota(jnp.int32, (own_count, cols), 0)
    owner_row = jnp.zeros((own_count, cols), jnp.int32)
    owner_lane = jnp.zeros((own_count, cols), jnp.int32)
    lane1 = lane[:1]
    local_lane = jnp.zeros((1, cols), jnp.int32)
    len_lane = jnp.zeros((1, cols), jnp.int32)
    lo_lane = jnp.zeros((1, cols), jnp.int32)
    sample_lane = jnp.zeros((own_count, cols), jnp.int32)
    for j in range(own_count):
        slot = slot_ref[sp_ref[first + j]]
        owner = lax.rem(lax.div(slot, prompts) - z + nz, nz)
        here = (lane >= j * heads) & (lane < (j + 1) * heads)
        owner_row = jnp.where(row == j, owner, owner_row)
        owner_lane = jnp.where(here, owner, owner_lane)
        sample_lane = jnp.where(here, j, sample_lane)
        local_lane = jnp.where(here[:1], lax.rem(slot, prompts), local_lane)
        len_lane = jnp.where(here[:1], len_ref[j], len_lane)
        lo_lane = jnp.where(here[:1], j * suffix, lo_lane)
    earlier = (owner_row == owner_lane) & (row < sample_lane)
    rank = jnp.sum(jnp.where(earlier, 1.0, 0.0), axis=0, keepdims=True).astype(jnp.int32)
    place = (owner_lane[:1] * sends + rank) * heads + (lane1 - sample_lane[:1] * heads)
    hot = lax.broadcasted_iota(jnp.int32, (packed_rows, cols), 0) == place

    def to_rows(values):
        return jnp.sum(jnp.where(hot, values.astype(F32), 0.0), axis=1, keepdims=True)

    hot_f = jnp.where(hot, 1.0, 0.0)
    q_load.wait()
    mine = dot(hot_f.astype(BF16), q_ref[...]).astype(BF16)
    tail = jnp.broadcast_to(to_rows(local_lane), (packed_rows, LANES)).astype(BF16)
    packed[:, :features] = mine
    packed[:, features:] = tail[:, : packed.shape[1] - features]
    recv[pl.ds((len(pairs) - 1) * rows, rows)] = packed[:rows]

    pl.semaphore_wait(barrier, nz * nx - 1)
    q_copies = []
    for k, (dz, dx) in enumerate(pairs):
        if k == len(pairs) - 1:
            q_copies.append(None)
            continue
        copy = pltpu.make_async_remote_copy(
            src_ref=packed.at[pl.ds(dz * rows, rows)],
            dst_ref=recv.at[pl.ds(k * rows, rows)],
            send_sem=q_send.at[k],
            recv_sem=q_recv.at[k],
            device_id=ahead(dz, dx),
            device_id_type=MESH,
        )
        copy.start()
        q_copies.append(copy)

    unpack[...] = hot_f.T.astype(BF16)
    lo = to_rows(lo_lane).astype(jnp.int32)
    hi = to_rows(lo_lane + len_lane).astype(jnp.int32)
    suf_copy.wait()
    scores = dot_t(packed[:, :features], sbuf[...]) * factor
    key = lax.broadcasted_iota(jnp.int32, scores.shape, 1)
    scores = jnp.where((key >= lo) & (key < hi), scores, -1e30)
    suf_max = jnp.max(scores, axis=1, keepdims=True)
    weights = jnp.exp2(scores - suf_max)
    suf_sum = jnp.sum(weights, axis=1, keepdims=True)
    suf_out[...] = dot(weights.astype(BF16), sbuf[:, :DL])

    kv_copy.wait()
    step = max(1, TILE_ROWS // rows)
    r_copies = [None] * len(pairs)
    for begin in range(0, len(pairs), step):
        end = min(begin + step, len(pairs))
        for k in range(begin, end):
            if k < len(pairs) - 1:
                q_copies[k].wait_recv()
        span = pl.ds(begin * rows, (end - begin) * rows)
        asked = recv[span, :features]
        local = recv[span, features : features + 1].astype(F32)
        scores = dot(asked, kbuf[0])
        for p in range(1, prompts):
            scores = jnp.where(local == float(p), dot(asked, kbuf[p]), scores)
        scores = scores * factor
        row_max = jnp.max(scores, axis=1, keepdims=True)
        weights = jnp.exp2(scores - row_max)
        row_sum = jnp.sum(weights, axis=1, keepdims=True)
        total = None
        for p in range(prompts):
            part = jnp.where(local == float(p), weights, 0.0).astype(BF16)
            part = dot_t(part, kbuf[p, :DL, :])
            total = part if total is None else total + part
        lse = row_max + jnp.log(row_sum) * LOG2E
        ret[span, :DL] = (total / row_sum).astype(BF16)
        place_of = lax.broadcasted_iota(jnp.int32, ((end - begin) * rows, LANES), 1)
        top, mid, low = split3(lse)
        tail = jnp.where(place_of == 0, top.astype(F32), jnp.where(place_of == 1, mid.astype(F32), low.astype(F32)))
        ret[span, DL:] = tail.astype(BF16)
        for k in range(begin, end):
            dz, dx = pairs[k]
            if k == len(pairs) - 1:
                got[pl.ds(k * rows, rows)] = ret[pl.ds(k * rows, rows)]
                continue
            copy = pltpu.make_async_remote_copy(
                src_ref=ret.at[pl.ds(k * rows, rows)],
                dst_ref=got.at[pl.ds(k * rows, rows)],
                send_sem=r_send.at[k],
                recv_sem=r_recv.at[k],
                device_id=behind(dz, dx),
                device_id_type=MESH,
            )
            copy.start()
            r_copies[k] = copy

    for dz in sorted(range(nz), key=lambda dz: (-min(dz, nz - dz), dz)):
        for k, pair in enumerate(pairs[:-1]):
            if pair[0] == dz:
                r_copies[k].wait_recv()
        span = pl.ds(dz * rows, rows)
        at = slice(dz * rows, (dz + 1) * rows)
        parts = []
        top = suf_max[at]
        for k, pair in enumerate(pairs):
            if pair[0] == dz:
                tail = got[pl.ds(k * rows, rows), DL:].astype(F32)
                lse = tail[:, 0:1] + tail[:, 1:2] + tail[:, 2:3]
                parts.append((k, lse))
                top = jnp.maximum(top, lse)
        share = jnp.exp2(suf_max[at] - top)
        total = share * suf_sum[at]
        numerator = share * suf_out[span, :]
        for k, lse in parts:
            share = jnp.exp2(lse - top)
            total = total + share
            numerator = numerator + share * got[pl.ds(k * rows, rows), :DL].astype(F32)
        result[span, :] = (numerator / total).astype(BF16)
    out_ref[...] = dot(unpack[...], result[...]).astype(BF16)
    for k in range(len(pairs) - 1):
        q_copies[k].wait_send()
        r_copies[k].wait_send()


def body(nz, nx, queries, prompt_cache, suffix_cache, suffix_len, sample_prompt, prompt_slot):
    own_count, heads, features = queries.shape
    prompts, tokens, _ = prompt_cache.shape
    suffix = suffix_cache.shape[1]
    sends = max(1, own_count // nz)
    devices = nz * nx
    cols = own_count * heads
    packed_rows = nz * sends * heads
    all_rows = devices * sends * heads
    wide = pl.cdiv(features + 1, LANES) * LANES
    vmem = pl.BlockSpec(memory_space=pltpu.VMEM)
    hbm = pl.BlockSpec(memory_space=pl.ANY)
    out = pl.pallas_call(
        functools.partial(kernel, nz, nx, own_count, heads, sends),
        out_shape=pltpu.VMEM((cols, DL), BF16),
        in_specs=[hbm] * 6,
        out_specs=vmem,
        scratch_shapes=[
            pltpu.VMEM((packed_rows, wide), BF16),
            pltpu.VMEM((all_rows, wide), BF16),
            pltpu.VMEM((all_rows, DL + LANES), BF16),
            pltpu.VMEM((all_rows, DL + LANES), BF16),
            pltpu.SMEM(suffix_len.shape, jnp.int32),
            pltpu.SMEM(sample_prompt.shape, jnp.int32),
            pltpu.SMEM(prompt_slot.shape, jnp.int32),
            pltpu.VMEM((cols, features), BF16),
            pltpu.VMEM((prompts, features, tokens), BF16),
            pltpu.VMEM((own_count * suffix, features), BF16),
            pltpu.VMEM((cols, packed_rows), BF16),
            pltpu.VMEM((packed_rows, DL), F32),
            pltpu.VMEM((packed_rows, DL), BF16),
            pltpu.SemaphoreType.DMA((6,)),
            pltpu.SemaphoreType.DMA((devices,)),
            pltpu.SemaphoreType.DMA((devices,)),
            pltpu.SemaphoreType.DMA((devices,)),
            pltpu.SemaphoreType.DMA((devices,)),
        ],
        compiler_params=pltpu.CompilerParams(collective_id=0, has_side_effects=True),
        name="latent_decode",
    )(
        queries.reshape(cols, features),
        jnp.swapaxes(prompt_cache, 1, 2),
        suffix_cache.reshape(own_count * suffix, features),
        suffix_len,
        sample_prompt,
        prompt_slot,
    )
    return out.reshape(own_count, heads, DL)


def solution(mesh):
    return jax.shard_map(
        functools.partial(body, mesh.shape["prompt"], mesh.shape["sample"]),
        mesh=mesh,
        in_specs=(
            P(("groups", "prompt", "sample"), "head", None),
            P(("groups", "prompt"), "sample", None),
            P(("groups", "prompt", "sample"), None, None),
            P(("groups", "prompt", "sample")),
            P("groups"),
            P("groups"),
        ),
        out_specs=P(("groups", "prompt", "sample"), "head", None),
        check_vma=False,
    )
```
